32 devices in a mesh: dp: 1 (over z), col: 4 (over y), row: 8 (over x, core).
Axes of the slice: x: 4, y: 4, z: 1, core: 2. Of those that a mesh axis runs over, the one named last changes fastest.
The devices are a block of a 4x4x8 slice.
Arguments:
- a_mat: bfloat16 [16384, 3072], P(('dp', 'row'), 'col')
- b_mat: bfloat16 [3072, 8192], P('row', 'col')
Outputs:
- output: bfloat16 [16384, 8192], P(('dp', 'row'), 'col')
All inputs are finite; a program needn't handle non-finite values.
Results may differ from the reference program's by a relative error of at most 0.001.
Values are sent between devices in bfloat16 or wider.
A program may use at most 768 MiB of HBM per device.

```python
import jax
import jax.numpy as jnp
from jax import lax

M_ROWS = 16384
K_INNER = 3072
N_COLS = 8192
ROW_BLOCK = 256


def setup_inputs(seed: int = 0, part: int = 0) -> dict:
    base_key = jax.random.key(seed)
    key_a = jax.random.fold_in(jax.random.fold_in(base_key, 1), part)
    key_b = jax.random.fold_in(base_key, 2)
    a_mat = jax.random.normal(key_a, (M_ROWS, K_INNER), jnp.float32).astype(jnp.bfloat16)
    b_mat = (jax.random.normal(key_b, (K_INNER, N_COLS), jnp.float32) * (K_INNER ** -0.5)).astype(jnp.bfloat16)
    return {"a_mat": a_mat, "b_mat": b_mat}


def reference(a_mat, b_mat):
    row_tiles = a_mat.reshape(M_ROWS // ROW_BLOCK, ROW_BLOCK, K_INNER)

    def tile_product(a_tile):
        return jnp.dot(a_tile, b_mat, preferred_element_type=jnp.float32).astype(jnp.bfloat16)

    out_tiles = lax.map(tile_product, row_tiles)
    return out_tiles.reshape(M_ROWS, N_COLS)
```

```python
import functools

import jax
import jax.numpy as jnp
from jax import lax
from jax.experimental import pallas as pl
from jax.experimental.pallas import tpu as pltpu
from jax.sharding import PartitionSpec as P

MESH = pl.DeviceIdType.MESH
PAIRS = 8
TILE_N = 512
FAR_TILE_N = 1024


def gather_multiply(num_rows, num_cols, a_hbm, b_hbm, c_ref, a_all, b_all, acc, la, lb, asend, arecv, fsend, frecv, bsend, brecv, gsend, grecv, psend, precv):
    row, col = lax.axis_index("row"), lax.axis_index("col")
    chip, core = row // 2, row % 2
    num_chips = num_rows // 2
    rows_a = a_hbm.shape[0]
    depth_b, width = b_hbm.shape
    chunk = rows_a // (2 * PAIRS)
    half = depth_b // 2

    up, down = {"col": (col + 1) % num_cols}, {"col": (col + num_cols - 1) % num_cols}
    east, west = {"row": (row + 2) % num_rows}, {"row": (row + num_rows - 2) % num_rows}
    partner = {"row": row + 1 - 2 * core}
    a_dirs, b_dirs = (up, down), (east, west)

    def remote(src, dst, send, recv, device):
        return pltpu.make_async_remote_copy(src_ref=src, dst_ref=dst, send_sem=send, recv_sem=recv, device_id=device, device_id_type=MESH)

    def a_at(slot, piece):
        return a_all.at[slot, pl.ds(pl.multiple_of(piece * chunk, chunk), chunk)]

    def a_own(way, piece):
        return remote(a_at(0, piece), a_at(1 + way, piece), asend.at[way, piece], arecv.at[way, piece], a_dirs[way])

    def a_far(way, piece):
        return remote(a_at(1 + way, piece), a_at(3, piece), fsend.at[piece], frecv.at[piece], a_dirs[way])

    chip_at = (chip, (chip + num_chips - 1) % num_chips, (chip + 1) % num_chips, (chip + 2) % num_chips)

    def b_at(slot, side, part):
        return b_all.at[chip_at[slot], pl.ds(pl.multiple_of(side * depth_b + part * half, half), half)]

    def b_own(way, part):
        piece = b_at(0, core, part)
        return remote(piece, piece, bsend.at[way, part], brecv.at[way, part], b_dirs[way])

    def b_far(way):
        piece = b_at(1 + way, core, way)
        return remote(piece, piece, gsend.at[way], grecv.at[way], b_dirs[way])

    def b_share(slot, part):
        piece = b_at(slot, core, part)
        return remote(piece, piece, psend.at[slot, part], precv.at[slot, part], partner)

    def a_load(piece):
        return pltpu.make_async_copy(a_hbm.at[pl.ds(piece * chunk, chunk)], a_at(0, piece), la.at[piece])

    def b_load(part):
        return pltpu.make_async_copy(b_hbm.at[pl.ds(part * half, half)], b_at(0, core, part), lb.at[part])

    even, odd = range(0, 2 * PAIRS, 2), range(1, 2 * PAIRS, 2)
    b_load(0).start()
    b_load(1).start()
    for piece in range(2 * PAIRS):
        a_load(piece).start()

    barrier = pltpu.get_barrier_semaphore()
    for device in (up, down, east, west, partner):
        pl.semaphore_signal(barrier, inc=1, device_id=device, device_id_type=MESH)
    pl.semaphore_wait(barrier, 5)

    b_load(0).wait()
    b_load(1).wait()
    for part in range(2):
        b_own(0, part).start()
        b_own(1, 1 - part).start()
    for piece in range(2 * PAIRS):
        a_load(piece).wait()
    for first, second in ((even, odd), (odd, even)):
        for plus, minus in zip(first, second):
            a_own(0, plus).start()
            a_own(1, minus).start()
    for part in range(2):
        b_share(0, part).start()

    for way in range(2):
        b_own(way, way).wait_recv()
        b_far(way).start()
        b_share(1 + way, way).start()

    @pl.loop(0, PAIRS)
    def _(pair):
        for way in range(2):
            piece = 2 * pair + way
            a_own(way, piece).wait_recv()
            a_far(way, piece).start()

    for way in range(2):
        b_own(way, 1 - way).wait_recv()
        b_share(1 + way, 1 - way).start()
    for way in range(2):
        b_far(way).wait_recv()
        b_share(3, way).start()
    for slot in range(4):
        for part in range(2):
            b_share(slot, part).wait_recv()

    block_at = (col, (col + num_cols - 1) % num_cols, (col + 1) % num_cols, (col + 2) % num_cols)

    def dot(slot, rows, cols):
        return jnp.dot(a_all[slot, rows, :], b_all[block_at[slot], :, cols], preferred_element_type=jnp.float32)

    @pl.loop(0, PAIRS // 2)
    def _(quad):
        for pair in (2 * quad, 2 * quad + 1):
            for way in range(2):
                a_own(way, 2 * pair + 1 - way).wait_recv()
        rows = pl.ds(pl.multiple_of(quad * 4 * chunk, 4 * chunk), 4 * chunk)

        @pl.loop(0, width // TILE_N)
        def _(tile):
            cols = pl.ds(pl.multiple_of(tile * TILE_N, TILE_N), TILE_N)
            acc[rows, cols] = dot(0, rows, cols) + dot(1, rows, cols) + dot(2, rows, cols)

    @pl.loop(0, PAIRS - 1)
    def _(pair):
        for way in range(2):
            a_far(way, 2 * pair + way).wait_recv()
        rows = pl.ds(pl.multiple_of(pair * 2 * chunk, 2 * chunk), 2 * chunk)

        @pl.loop(0, width // FAR_TILE_N)
        def _(tile):
            cols = pl.ds(pl.multiple_of(tile * FAR_TILE_N, FAR_TILE_N), FAR_TILE_N)
            c_ref[rows, cols] = (acc[rows, cols] + dot(3, rows, cols)).astype(c_ref.dtype)

    for way in range(2):
        a_far(way, 2 * (PAIRS - 1) + way).wait_recv()

    @pl.loop(0, 2 * PAIRS)
    def _(piece):
        for way in range(2):
            a_own(way, piece).wait_send()

    @pl.loop(0, PAIRS)
    def _(pair):
        for way in range(2):
            a_far(way, 2 * pair + way).wait_send()

    for way in range(2):
        for part in range(2):
            b_own(way, part).wait_send()
        b_far(way).wait_send()
    for slot in range(4):
        for part in range(2):
            b_share(slot, part).wait_send()


def finish(num_cols, c_done, a_all, b_all, acc, c_hbm, c_last, sems):
    rows_c = c_hbm.shape[0]
    last = rows_c // PAIRS
    done = pl.ds(0, rows_c - last)
    tail = pl.ds(rows_c - last, last)
    early = pltpu.make_async_copy(c_done.at[done], c_hbm.at[done], sems.at[0])
    early.start()
    block = (lax.axis_index("col") + 2) % num_cols
    c_last[...] = (acc[tail] + jnp.dot(a_all[3, tail, :], b_all[block], preferred_element_type=jnp.float32)).astype(c_last.dtype)
    late = pltpu.make_async_copy(c_last, c_hbm.at[tail], sems.at[1])
    late.start()
    early.wait()
    late.wait()


def solution(mesh):
    num_rows, num_cols = mesh.shape["row"], mesh.shape["col"]

    def local_product(a_blk, b_blk):
        rows, depth = a_blk.shape
        depth_b, width = b_blk.shape
        dma = pltpu.SemaphoreType.DMA
        vmem = pl.BlockSpec(memory_space=pltpu.VMEM)
        hbm = pl.BlockSpec(memory_space=pltpu.HBM)
        far_flops = 2 * rows * width * depth // PAIRS
        gathered = pl.pallas_call(
            functools.partial(gather_multiply, num_rows, num_cols),
            out_shape=(
                pltpu.VMEM((rows, width), jnp.bfloat16),
                pltpu.VMEM((4, rows, depth), jnp.bfloat16),
                pltpu.VMEM((num_rows // 2, 2 * depth_b, width), jnp.bfloat16),
                pltpu.VMEM((rows, width), jnp.float32),
            ),
            in_specs=[hbm] * 2,
            out_specs=(vmem,) * 4,
            scratch_shapes=[
                dma((2 * PAIRS,)),
                dma((2,)),
                dma((2, 2 * PAIRS)),
                dma((2, 2 * PAIRS)),
                dma((2 * PAIRS,)),
                dma((2 * PAIRS,)),
                dma((2, 2)),
                dma((2, 2)),
                dma((2,)),
                dma((2,)),
                dma((4, 2)),
                dma((4, 2)),
            ],
            cost_estimate=pl.CostEstimate(flops=2 * rows * width * depth * num_cols - far_flops, bytes_accessed=2 * (rows * depth + depth_b * width), transcendentals=0),
            compiler_params=pltpu.CompilerParams(collective_id=0, has_side_effects=True, vmem_limit_bytes=8 * 1024 * 1024),
            name="gather_multiply",
        )(a_blk, b_blk)
        return pl.pallas_call(
            functools.partial(finish, num_cols),
            out_shape=jax.ShapeDtypeStruct((rows, width), jnp.bfloat16),
            in_specs=[vmem] * 4,
            out_specs=hbm,
            scratch_shapes=[pltpu.VMEM((rows // PAIRS, width), jnp.bfloat16), dma((2,))],
            cost_estimate=pl.CostEstimate(flops=far_flops, bytes_accessed=2 * rows * width, transcendentals=0),
            compiler_params=pltpu.CompilerParams(vmem_limit_bytes=8 * 1024 * 1024),
            name="finish",
        )(*(pltpu.with_memory_space_constraint(part, pltpu.VMEM) for part in gathered))

    return jax.shard_map(local_product, mesh=mesh, in_specs=(P(("dp", "row"), "col"), P("row", "col")), out_specs=P(("dp", "row"), "col"), check_vma=False)
```

```python
import functools

import jax
import jax.numpy as jnp
from jax import lax
from jax.experimental import pallas as pl
from jax.experimental.pallas import tpu as pltpu
from jax.sharding import PartitionSpec as P

MESH = pl.DeviceIdType.MESH
BLOCK = 512
PIECE = 256
LAST = 128
TILE_N = 512
FAR_TILE_N = 1024


def own_plan(rows):
    mid = rows // 2
    return (
        ((0, LAST), (LAST, mid - LAST), (mid, mid // 2), (mid + mid // 2, mid // 2)),
        ((rows - LAST, LAST), (mid, mid - LAST), (0, mid // 2), (mid // 2, mid // 2)),
    )


def far_plan(rows):
    mid = rows // 2
    sizes = [PIECE] * (mid // PIECE - 1) + [LAST] * (PIECE // LAST)
    starts = [sum(sizes[:k]) for k in range(len(sizes))]
    return tuple(zip(starts, sizes)), tuple((rows - start - size, size) for start, size in zip(starts, sizes))


def gather_multiply(num_rows, num_cols, a_hbm, b_hbm, c_ref, a_all, b_all, acc, la, lb, asend, arecv, fsend, frecv, bsend, brecv, gsend, grecv, psend, precv, joined, ready, go):
    row, col = lax.axis_index("row"), lax.axis_index("col")
    chip, core = row // 2, row % 2
    num_chips = num_rows // 2
    rows_a = a_hbm.shape[0]
    depth_b, width = b_hbm.shape
    own, far = own_plan(rows_a), far_plan(rows_a)
    pieces = len(far[0])
    half = depth_b // 2

    up, down = {"col": (col + 1) % num_cols}, {"col": (col + num_cols - 1) % num_cols}
    east, west = {"row": (row + 2) % num_rows}, {"row": (row + num_rows - 2) % num_rows}
    partner = {"row": row + 1 - 2 * core}
    a_dirs, b_dirs = (up, down), (east, west)

    def remote(src, dst, send, recv, device):
        return pltpu.make_async_remote_copy(src_ref=src, dst_ref=dst, send_sem=send, recv_sem=recv, device_id=device, device_id_type=MESH)

    def a_at(slot, place):
        return a_all.at[slot, pl.ds(*place)]

    def a_own(way, k):
        return remote(a_at(0, own[way][k]), a_at(1 + way, own[way][k]), asend.at[way, k], arecv.at[way, k], a_dirs[way])

    def a_far(way, k):
        return remote(a_at(1 + way, far[way][k]), a_at(3, far[way][k]), fsend.at[way, k], frecv.at[way, k], a_dirs[way])

    chip_at = (chip, (chip + num_chips - 1) % num_chips, (chip + 1) % num_chips, (chip + 2) % num_chips)

    def b_at(slot, side, part):
        return b_all.at[chip_at[slot], pl.ds(pl.multiple_of(side * depth_b + part * half, half), half)]

    def b_own(way, part):
        piece = b_at(0, core, part)
        return remote(piece, piece, bsend.at[way, part], brecv.at[way, part], b_dirs[way])

    def b_far(way):
        piece = b_at(1 + way, core, way)
        return remote(piece, piece, gsend.at[way], grecv.at[way], b_dirs[way])

    def b_share(slot, part):
        piece = b_at(slot, core, part)
        return remote(piece, piece, psend.at[slot, part], precv.at[slot, part], partner)

    def a_load(way, k):
        return pltpu.make_async_copy(a_hbm.at[pl.ds(*own[way][k])], a_at(0, own[way][k]), la.at[way, k])

    def b_load(part):
        return pltpu.make_async_copy(b_hbm.at[pl.ds(part * half, half)], b_at(0, core, part), lb.at[part])

    for k in range(2):
        for way in range(2):
            a_load(way, k).start()
    b_load(0).start()
    b_load(1).start()

    barrier = pltpu.get_barrier_semaphore()
    hub, after, across, before = range(num_cols)

    def signal(sem, *devices):
        for device in devices:
            pl.semaphore_signal(sem, inc=1, device_id=device, device_id_type=MESH)

    signal(barrier, up, down)

    @pl.when(col == hub)
    def _():
        signal(barrier, east, west, partner)
        pl.semaphore_wait(barrier, 5)

    @pl.when(col != hub)
    def _():
        pl.semaphore_wait(barrier, 2)

    for k in range(4):
        for way in range(2):
            if k < 2:
                a_load(way, k).wait()
            a_own(way, k).start()

    @pl.when(col == hub)
    def _():
        pl.semaphore_wait(joined, 2)
        signal(ready, east, west, partner)
        pl.semaphore_wait(ready, 3)
        signal(go, up, down)

    @pl.when(col == before)
    def _():
        signal(joined, up)
        pl.semaphore_wait(go, 1)

    @pl.when(col == after)
    def _():
        signal(joined, down)
        pl.semaphore_wait(go, 1)
        signal(go, up)

    @pl.when(col == across)
    def _():
        pl.semaphore_wait(go, 1)

    b_load(0).wait()
    b_load(1).wait()
    for part in range(2):
        b_own(0, part).start()
        b_own(1, 1 - part).start()
    for part in range(2):
        b_share(0, part).start()

    for way in range(2):
        b_own(way, way).wait_recv()
        b_far(way).start()
        b_share(1 + way, way).start()

    for way in range(2):
        for k in range(2):
            a_own(way, k).wait_recv()
        for k in range(pieces):
            a_far(way, k).start()

    for way in range(2):
        b_own(way, 1 - way).wait_recv()
        b_share(1 + way, 1 - way).start()
    for way in range(2):
        b_far(way).wait_recv()
        b_share(3, way).start()
    for slot in range(4):
        for part in range(2):
            b_share(slot, part).wait_recv()

    block_at = (col, (col + num_cols - 1) % num_cols, (col + 1) % num_cols, (col + 2) % num_cols)

    def dot(slot, rows, cols):
        return jnp.dot(a_all[slot, rows, :], b_all[block_at[slot], :, cols], preferred_element_type=jnp.float32)

    def near(block):
        rows = pl.ds(pl.multiple_of(block * BLOCK, BLOCK), BLOCK)

        @pl.loop(0, width // TILE_N)
        def _(tile):
            cols = pl.ds(pl.multiple_of(tile * TILE_N, TILE_N), TILE_N)
            acc[rows, cols] = dot(0, rows, cols) + dot(1, rows, cols) + dot(2, rows, cols)

    def away(start, size):
        rows = pl.ds(start, size)

        @pl.loop(0, width // FAR_TILE_N)
        def _(tile):
            cols = pl.ds(pl.multiple_of(tile * FAR_TILE_N, FAR_TILE_N), FAR_TILE_N)
            c_ref[rows, cols] = (acc[rows, cols] + dot(3, rows, cols)).astype(c_ref.dtype)

    blocks = rows_a // BLOCK
    for k in range(2):
        for way in range(2):
            a_own(way, 2 + k).wait_recv()

        @pl.loop(0, blocks // 2)
        def _(turn):
            near(turn * 2 + k)

    for way in range(2):
        for k in range(4):
            a_own(way, k).wait_send()
        for part in range(2):
            b_own(way, part).wait_send()
        b_far(way).wait_send()
    for slot in range(4):
        for part in range(2):
            b_share(slot, part).wait_send()

    for k in range(pieces):
        for way in range(2):
            a_far(way, k).wait_recv()
            if k < pieces - 1:
                away(*far[way][k])
    for k in range(pieces):
        for way in range(2):
            a_far(way, k).wait_send()


def finish(num_cols, c_done, a_all, b_all, acc, c_hbm, c_last, sems):
    rows_c = c_hbm.shape[0]
    mid = rows_c // 2
    tail = pl.ds(mid - LAST, 2 * LAST)
    copies = []
    for k, rows in enumerate((pl.ds(0, mid - LAST), pl.ds(mid + LAST, mid - LAST))):
        copies.append(pltpu.make_async_copy(c_done.at[rows], c_hbm.at[rows], sems.at[k]))
        copies[-1].start()
    block = (lax.axis_index("col") + 2) % num_cols
    c_last[...] = (acc[tail] + jnp.dot(a_all[3, tail, :], b_all[block], preferred_element_type=jnp.float32)).astype(c_last.dtype)
    copies.append(pltpu.make_async_copy(c_last, c_hbm.at[tail], sems.at[2]))
    copies[-1].start()
    for copy in copies:
        copy.wait()


def solution(mesh):
    num_rows, num_cols = mesh.shape["row"], mesh.shape["col"]

    def local_product(a_blk, b_blk):
        rows, depth = a_blk.shape
        depth_b, width = b_blk.shape
        dma = pltpu.SemaphoreType.DMA
        vmem = pl.BlockSpec(memory_space=pltpu.VMEM)
        hbm = pl.BlockSpec(memory_space=pltpu.HBM)
        far_flops = 4 * LAST * width * depth
        pieces = len(far_plan(rows)[0])
        gathered = pl.pallas_call(
            functools.partial(gather_multiply, num_rows, num_cols),
            out_shape=(
                pltpu.VMEM((rows, width), jnp.bfloat16),
                pltpu.VMEM((4, rows, depth), jnp.bfloat16),
                pltpu.VMEM((num_rows // 2, 2 * depth_b, width), jnp.bfloat16),
                pltpu.VMEM((rows, width), jnp.float32),
            ),
            in_specs=[hbm] * 2,
            out_specs=(vmem,) * 4,
            scratch_shapes=[
                dma((2, 2)),
                dma((2,)),
                dma((2, 4)),
                dma((2, 4)),
                dma((2, pieces)),
                dma((2, pieces)),
                dma((2, 2)),
                dma((2, 2)),
                dma((2,)),
                dma((2,)),
                dma((4, 2)),
                dma((4, 2)),
                pltpu.SemaphoreType.REGULAR,
                pltpu.SemaphoreType.REGULAR,
                pltpu.SemaphoreType.REGULAR,
            ],
            cost_estimate=pl.CostEstimate(flops=2 * rows * width * depth * num_cols - far_flops, bytes_accessed=2 * (rows * depth + depth_b * width), transcendentals=0),
            compiler_params=pltpu.CompilerParams(collective_id=0, has_side_effects=True, vmem_limit_bytes=8 * 1024 * 1024),
            name="gather_multiply",
        )(a_blk, b_blk)
        return pl.pallas_call(
            functools.partial(finish, num_cols),
            out_shape=jax.ShapeDtypeStruct((rows, width), jnp.bfloat16),
            in_specs=[vmem] * 4,
            out_specs=hbm,
            scratch_shapes=[pltpu.VMEM((2 * LAST, width), jnp.bfloat16), dma((3,))],
            cost_estimate=pl.CostEstimate(flops=far_flops, bytes_accessed=2 * rows * width, transcendentals=0),
            compiler_params=pltpu.CompilerParams(vmem_limit_bytes=8 * 1024 * 1024),
            name="finish",
        )(*(pltpu.with_memory_space_constraint(part, pltpu.VMEM) for part in gathered))

    return jax.shard_map(local_product, mesh=mesh, in_specs=(P(("dp", "row"), "col"), P("row", "col")), out_specs=P(("dp", "row"), "col"), check_vma=False)
```

```python
import functools

import jax
import jax.numpy as jnp
from jax import lax
from jax.experimental import pallas as pl
from jax.experimental.pallas import tpu as pltpu
from jax.sharding import PartitionSpec as P

MESH = pl.DeviceIdType.MESH
BLOCK = 512
PIECE = 256
LAST = 128
SPARED = (32, 48)
TILE_N = 512
FAR_TILE_N = 1024


def own_plan(rows):
    mid = rows // 2
    return (
        ((0, LAST), (LAST, mid - LAST), (mid, mid // 2), (mid + mid // 2, mid // 2)),
        ((rows - LAST, LAST), (mid, mid - LAST), (mid // 2, mid // 2), (0, mid // 2)),
    )


def far_plan(rows):
    mid = rows // 2
    plans = []
    for spared in SPARED:
        sizes = [PIECE] * (mid // PIECE - 1) + [LAST] * (PIECE // LAST - 1) + [LAST - spared, spared]
        plans.append([(sum(sizes[:k]), size) for k, size in enumerate(sizes)])
    return plans[0], [(rows - start - size, size) for start, size in plans[1]]


def gather_multiply(num_rows, num_cols, a_hbm, b_hbm, c_ref, a_all, b_all, acc, la, lb, asend, arecv, fsend, frecv, esend, bsend, brecv, gsend, grecv, psend, precv, peer, joined, ready, go):
    row, col = lax.axis_index("row"), lax.axis_index("col")
    chip, core = row // 2, row % 2
    num_chips = num_rows // 2
    rows_a = a_hbm.shape[0]
    depth_b, width = b_hbm.shape
    own, far = own_plan(rows_a), far_plan(rows_a)
    pieces = len(far[0])
    half = depth_b // 2

    up, down = {"col": (col + 1) % num_cols}, {"col": (col + num_cols - 1) % num_cols}
    east, west = {"row": (row + 2) % num_rows}, {"row": (row + num_rows - 2) % num_rows}
    partner = {"row": row + 1 - 2 * core}
    a_dirs, b_dirs = (up, down), (east, west)

    def remote(src, dst, send, recv, device):
        return pltpu.make_async_remote_copy(src_ref=src, dst_ref=dst, send_sem=send, recv_sem=recv, device_id=device, device_id_type=MESH)

    def a_at(slot, place):
        return a_all.at[slot, pl.ds(*place)]

    def a_own(way, k):
        return remote(a_at(0, own[way][k]), a_at(1 + way, own[way][k]), asend.at[way, k], arecv.at[way, k], a_dirs[way])

    def a_far(way, k):
        return remote(a_at(1 + way, far[way][k]), a_at(3, far[way][k]), fsend.at[way, k], frecv.at[way, k], a_dirs[way])

    def a_extra(way):
        place = far[1 - way][-1]
        return remote(a_at(1 + way, place), a_at(3, place), esend.at[way], frecv.at[1 - way, pieces - 1], a_dirs[way])

    chip_at = (chip, (chip + num_chips - 1) % num_chips, (chip + 1) % num_chips, (chip + 2) % num_chips)

    def b_at(slot, side, part):
        return b_all.at[chip_at[slot], pl.ds(pl.multiple_of(side * depth_b + part * half, half), half)]

    def b_own(way, part):
        piece = b_at(0, core, part)
        return remote(piece, piece, bsend.at[way, part], brecv.at[way, part], b_dirs[way])

    def b_far(way):
        piece = b_at(1 + way, core, way)
        return remote(piece, piece, gsend.at[way], grecv.at[way], b_dirs[way])

    def b_share(slot, part):
        piece = b_at(slot, core, part)
        return remote(piece, piece, psend.at[slot, part], precv.at[slot, part], partner)

    def a_load(way, k):
        return pltpu.make_async_copy(a_hbm.at[pl.ds(*own[way][k])], a_at(0, own[way][k]), la.at[way, k])

    def b_load(part):
        return pltpu.make_async_copy(b_hbm.at[pl.ds(part * half, half)], b_at(0, core, part), lb.at[part])

    for k in range(2):
        for way in range(2):
            a_load(way, k).start()
    b_load(0).start()
    b_load(1).start()

    barrier = pltpu.get_barrier_semaphore()
    hub, after, across, before = range(num_cols)

    def signal(sem, *devices):
        for device in devices:
            pl.semaphore_signal(sem, inc=1, device_id=device, device_id_type=MESH)

    def send_own(way, between):
        for k in range(2):
            a_load(way, k).wait()
            a_own(way, k).start()
        for k in range(2):
            a_load(1 - way, k).wait()
        for k in range(2, 4):
            a_own(way, k).start()
        between()
        for k in range(4):
            a_own(1 - way, k).start()

    signal(barrier, up)

    @pl.when(col == hub)
    def _():
        signal(barrier, down, east, west, partner)

    @pl.when(jnp.logical_or(col == after, col == across))
    def _():
        pl.semaphore_wait(barrier, 1)
        signal(peer, down)
        send_own(1, lambda: pl.semaphore_wait(peer, 1))

    @pl.when(col == before)
    def _():
        pl.semaphore_wait(barrier, 2)
        signal(peer, down)
        send_own(0, lambda: None)

    @pl.when(col == hub)
    def _():
        pl.semaphore_wait(peer, 1)
        send_own(0, lambda: pl.semaphore_wait(barrier, 4))

    @pl.when(col == hub)
    def _():
        pl.semaphore_wait(joined, 2)
        signal(ready, east, west, partner)
        pl.semaphore_wait(ready, 3)
        signal(go, up, down)

    @pl.when(col == before)
    def _():
        signal(joined, up)
        pl.semaphore_wait(go, 1)

    @pl.when(col == after)
    def _():
        signal(joined, down)
        pl.semaphore_wait(go, 1)
        signal(go, up)

    @pl.when(col == across)
    def _():
        pl.semaphore_wait(go, 1)

    b_load(0).wait()
    b_load(1).wait()
    for part in range(2):
        b_own(0, part).start()
        b_own(1, 1 - part).start()
    for part in range(2):
        b_share(0, part).start()

    for way in range(2):
        b_own(way, way).wait_recv()
        b_far(way).start()
        b_share(1 + way, way).start()

    for way in range(2):
        for k in range(2):
            a_own(way, k).wait_recv()
        for k in range(pieces - 1):
            a_far(way, k).start()

    for way in range(2):
        b_own(way, 1 - way).wait_recv()
        b_share(1 + way, 1 - way).start()
    for way in range(2):
        b_far(way).wait_recv()
        b_share(3, way).start()
    for slot in range(4):
        for part in range(2):
            b_share(slot, part).wait_recv()

    for way in range(2):
        a_own(way, 2).wait_recv()

    def spared(act):
        @pl.when(col != before)
        def _():
            act(a_far(0, pieces - 1))

        @pl.when(col != hub)
        def _():
            act(a_far(1, pieces - 1))

        @pl.when(col == after)
        def _():
            act(a_extra(1))

        @pl.when(col == across)
        def _():
            act(a_extra(0))

    spared(lambda copy: copy.start())

    block_at = (col, (col + num_cols - 1) % num_cols, (col + 1) % num_cols, (col + 2) % num_cols)

    def dot(slot, rows, cols):
        return jnp.dot(a_all[slot, rows, :], b_all[block_at[slot], :, cols], preferred_element_type=jnp.float32)

    def near(block):
        rows = pl.ds(pl.multiple_of(block * BLOCK, BLOCK), BLOCK)

        @pl.loop(0, width // TILE_N)
        def _(tile):
            cols = pl.ds(pl.multiple_of(tile * TILE_N, TILE_N), TILE_N)
            acc[rows, cols] = dot(0, rows, cols) + dot(1, rows, cols) + dot(2, rows, cols)

    def away(start, size):
        rows = pl.ds(start, size)

        @pl.loop(0, width // FAR_TILE_N)
        def _(tile):
            cols = pl.ds(pl.multiple_of(tile * FAR_TILE_N, FAR_TILE_N), FAR_TILE_N)
            c_ref[rows, cols] = (acc[rows, cols] + dot(3, rows, cols)).astype(c_ref.dtype)

    quarter = rows_a // (4 * BLOCK)
    for first, second in ((1, 2), (0, 3)):
        if first == 0:
            for way in range(2):
                a_own(way, 3).wait_recv()

        @pl.loop(0, 2 * quarter)
        def _(turn):
            near(first * quarter + turn % quarter + (turn // quarter) * (second - first) * quarter)

    for way in range(2):
        for k in range(4):
            a_own(way, k).wait_send()
        for part in range(2):
            b_own(way, part).wait_send()
        b_far(way).wait_send()
    for slot in range(4):
        for part in range(2):
            b_share(slot, part).wait_send()

    for k in range(pieces):
        for way in range(2):
            a_far(way, k).wait_recv()
            if k < pieces - 2:
                away(*far[way][k])
    for k in range(pieces - 1):
        for way in range(2):
            a_far(way, k).wait_send()
    spared(lambda copy: copy.wait_send())


def finish(num_cols, c_done, a_all, b_all, acc, c_hbm, c_last, sems):
    rows_c = c_hbm.shape[0]
    mid = rows_c // 2
    tail = pl.ds(mid - LAST, 2 * LAST)
    copies = []
    for k, rows in enumerate((pl.ds(0, mid - LAST), pl.ds(mid + LAST, mid - LAST))):
        copies.append(pltpu.make_async_copy(c_done.at[rows], c_hbm.at[rows], sems.at[k]))
        copies[-1].start()
    block = (lax.axis_index("col") + 2) % num_cols
    c_last[...] = (acc[tail] + jnp.dot(a_all[3, tail, :], b_all[block], preferred_element_type=jnp.float32)).astype(c_last.dtype)
    copies.append(pltpu.make_async_copy(c_last, c_hbm.at[tail], sems.at[2]))
    copies[-1].start()
    for copy in copies:
        copy.wait()


def solution(mesh):
    num_rows, num_cols = mesh.shape["row"], mesh.shape["col"]

    def local_product(a_blk, b_blk):
        rows, depth = a_blk.shape
        depth_b, width = b_blk.shape
        dma = pltpu.SemaphoreType.DMA
        vmem = pl.BlockSpec(memory_space=pltpu.VMEM)
        hbm = pl.BlockSpec(memory_space=pltpu.HBM)
        far_flops = 4 * LAST * width * depth
        pieces = len(far_plan(rows)[0])
        gathered = pl.pallas_call(
            functools.partial(gather_multiply, num_rows, num_cols),
            out_shape=(
                pltpu.VMEM((rows, width), jnp.bfloat16),
                pltpu.VMEM((4, rows, depth), jnp.bfloat16),
                pltpu.VMEM((num_rows // 2, 2 * depth_b, width), jnp.bfloat16),
                pltpu.VMEM((rows, width), jnp.float32),
            ),
            in_specs=[hbm] * 2,
            out_specs=(vmem,) * 4,
            scratch_shapes=[
                dma((2, 2)),
                dma((2,)),
                dma((2, 4)),
                dma((2, 4)),
                dma((2, pieces)),
                dma((2, pieces)),
                dma((2,)),
                dma((2, 2)),
                dma((2, 2)),
                dma((2,)),
                dma((2,)),
                dma((4, 2)),
                dma((4, 2)),
                pltpu.SemaphoreType.REGULAR,
                pltpu.SemaphoreType.REGULAR,
                pltpu.SemaphoreType.REGULAR,
                pltpu.SemaphoreType.REGULAR,
            ],
            cost_estimate=pl.CostEstimate(flops=2 * rows * width * depth * num_cols - far_flops, bytes_accessed=2 * (rows * depth + depth_b * width), transcendentals=0),
            compiler_params=pltpu.CompilerParams(collective_id=0, has_side_effects=True, vmem_limit_bytes=8 * 1024 * 1024),
            name="gather_multiply",
        )(a_blk, b_blk)
        return pl.pallas_call(
            functools.partial(finish, num_cols),
            out_shape=jax.ShapeDtypeStruct((rows, width), jnp.bfloat16),
            in_specs=[vmem] * 4,
            out_specs=hbm,
            scratch_shapes=[pltpu.VMEM((2 * LAST, width), jnp.bfloat16), dma((3,))],
            cost_estimate=pl.CostEstimate(flops=far_flops, bytes_accessed=2 * rows * width, transcendentals=0),
            compiler_params=pltpu.CompilerParams(vmem_limit_bytes=8 * 1024 * 1024),
            name="finish",
        )(*(pltpu.with_memory_space_constraint(part, pltpu.VMEM) for part in gathered))

    return jax.shard_map(local_product, mesh=mesh, in_specs=(P(("dp", "row"), "col"), P("row", "col")), out_specs=P(("dp", "row"), "col"), check_vma=False)
```

```python
import functools

import jax
import jax.numpy as jnp
from jax import lax
from jax.experimental import pallas as pl
from jax.experimental.pallas import tpu as pltpu
from jax.sharding import PartitionSpec as P

MESH = pl.DeviceIdType.MESH
BLOCK = 512
PIECE = 256
LAST = 128
SPARED = (32, 32)
TILE_N = 512
FAR_TILE_N = 1024


def own_plan(rows):
    mid = rows // 2
    return (
        ((0, LAST), (LAST, mid - LAST), (mid, mid // 2), (mid + mid // 2, mid // 2)),
        ((rows - LAST, LAST), (mid, mid - LAST), (mid // 2, mid // 2), (0, mid // 2)),
    )


def far_plan(rows):
    mid = rows // 2
    plans = []
    for spared in SPARED:
        sizes = [PIECE] * (mid // PIECE - 1) + [LAST] * (PIECE // LAST - 1) + [LAST - spared, spared]
        plans.append([(sum(sizes[:k]), size) for k, size in enumerate(sizes)])
    return plans[0], [(rows - start - size, size) for start, size in plans[1]]


def gather_multiply(num_rows, num_cols, a_hbm, b_hbm, c_ref, a_all, b_all, acc, la, lb, asend, arecv, fsend, frecv, esend, bsend, brecv, gsend, grecv, psend, precv, peer, joined, ready, go):
    row, col = lax.axis_index("row"), lax.axis_index("col")
    chip, core = row // 2, row % 2
    num_chips = num_rows // 2
    rows_a = a_hbm.shape[0]
    depth_b, width = b_hbm.shape
    own, far = own_plan(rows_a), far_plan(rows_a)
    pieces = len(far[0])
    half = depth_b // 2

    up, down = {"col": (col + 1) % num_cols}, {"col": (col + num_cols - 1) % num_cols}
    east, west = {"row": (row + 2) % num_rows}, {"row": (row + num_rows - 2) % num_rows}
    partner = {"row": row + 1 - 2 * core}
    a_dirs, b_dirs = (up, down), (east, west)

    def remote(src, dst, send, recv, device):
        return pltpu.make_async_remote_copy(src_ref=src, dst_ref=dst, send_sem=send, recv_sem=recv, device_id=device, device_id_type=MESH)

    def a_at(slot, place):
        return a_all.at[slot, pl.ds(*place)]

    def a_own(way, k):
        source = a_hbm.at[pl.ds(*own[way][0])] if k == 0 else a_at(0, own[way][k])
        return remote(source, a_at(1 + way, own[way][k]), asend.at[way, k], arecv.at[way, k], a_dirs[way])

    def a_far(way, k):
        return remote(a_at(1 + way, far[way][k]), a_at(3, far[way][k]), fsend.at[way, k], frecv.at[way, k], a_dirs[way])

    def a_extra(way):
        place = far[1 - way][-1]
        return remote(a_at(1 + way, place), a_at(3, place), esend.at[way], frecv.at[1 - way, pieces - 1], a_dirs[way])

    chip_at = (chip, (chip + num_chips - 1) % num_chips, (chip + 1) % num_chips, (chip + 2) % num_chips)

    def b_at(slot, side, part):
        return b_all.at[chip_at[slot], pl.ds(pl.multiple_of(side * depth_b + part * half, half), half)]

    def b_own(way, part):
        piece = b_at(0, core, part)
        return remote(piece, piece, bsend.at[way, part], brecv.at[way, part], b_dirs[way])

    def b_far(way):
        piece = b_at(1 + way, core, way)
        return remote(piece, piece, gsend.at[way], grecv.at[way], b_dirs[way])

    def b_share(slot, part):
        piece = b_at(slot, core, part)
        return remote(piece, piece, psend.at[slot, part], precv.at[slot, part], partner)

    def a_load(way, k):
        return pltpu.make_async_copy(a_hbm.at[pl.ds(*own[way][k])], a_at(0, own[way][k]), la.at[way, k])

    def b_load(part):
        return pltpu.make_async_copy(b_hbm.at[pl.ds(part * half, half)], b_at(0, core, part), lb.at[part])

    barrier = pltpu.get_barrier_semaphore()
    hub, after, across, before = range(num_cols)

    def signal(sem, *devices):
        for device in devices:
            pl.semaphore_signal(sem, inc=1, device_id=device, device_id_type=MESH)

    def send_own(way, between):
        a_own(way, 0).start()
        for k in range(2):
            a_load(way, k).wait()
        a_own(way, 1).start()
        for k in range(2):
            a_load(1 - way, k).wait()
        for k in range(2, 4):
            a_own(way, k).start()
        between()
        for k in range(4):
            a_own(1 - way, k).start()

    signal(barrier, up)

    @pl.when(col == hub)
    def _():
        signal(barrier, down, east, west, partner)

    for k in range(2):
        for way in range(2):
            a_load(way, k).start()

    @pl.when(jnp.logical_or(col == after, col == across))
    def _():
        pl.semaphore_wait(barrier, 1)
        signal(peer, down)
        send_own(1, lambda: pl.semaphore_wait(peer, 1))

    @pl.when(col == before)
    def _():
        pl.semaphore_wait(barrier, 2)
        signal(peer, down)
        send_own(0, lambda: None)

    @pl.when(col == hub)
    def _():
        pl.semaphore_wait(peer, 1)
        send_own(0, lambda: pl.semaphore_wait(barrier, 4))

    b_load(0).start()
    b_load(1).start()

    @pl.when(col == hub)
    def _():
        pl.semaphore_wait(joined, 2)
        signal(ready, east, west, partner)
        pl.semaphore_wait(ready, 3)
        signal(go, up, down)

    @pl.when(col == before)
    def _():
        signal(joined, up)
        pl.semaphore_wait(go, 1)

    @pl.when(col == after)
    def _():
        signal(joined, down)
        pl.semaphore_wait(go, 1)
        signal(go, up)

    @pl.when(col == across)
    def _():
        pl.semaphore_wait(go, 1)

    b_load(0).wait()
    b_load(1).wait()
    for part in range(2):
        b_own(0, part).start()
        b_own(1, 1 - part).start()
    for part in range(2):
        b_share(0, part).start()

    for way in range(2):
        b_own(way, way).wait_recv()
        b_far(way).start()
        b_share(1 + way, way).start()

    for way in range(2):
        for k in range(2):
            a_own(way, k).wait_recv()
        for k in range(pieces - 1):
            a_far(way, k).start()

    for way in range(2):
        b_own(way, 1 - way).wait_recv()
        b_share(1 + way, 1 - way).start()
    for way in range(2):
        b_far(way).wait_recv()
        b_share(3, way).start()
    for slot in range(4):
        for part in range(2):
            b_share(slot, part).wait_recv()

    for way in range(2):
        a_own(way, 2).wait_recv()

    def spared(act):
        @pl.when(col != before)
        def _():
            act(a_far(0, pieces - 1))

        @pl.when(col != hub)
        def _():
            act(a_far(1, pieces - 1))

        @pl.when(col == after)
        def _():
            act(a_extra(1))

        @pl.when(col == across)
        def _():
            act(a_extra(0))

    spared(lambda copy: copy.start())

    block_at = (col, (col + num_cols - 1) % num_cols, (col + 1) % num_cols, (col + 2) % num_cols)

    def dot(slot, rows, cols):
        return jnp.dot(a_all[slot, rows, :], b_all[block_at[slot], :, cols], preferred_element_type=jnp.float32)

    def near(block):
        rows = pl.ds(pl.multiple_of(block * BLOCK, BLOCK), BLOCK)

        @pl.loop(0, width // TILE_N)
        def _(tile):
            cols = pl.ds(pl.multiple_of(tile * TILE_N, TILE_N), TILE_N)
            acc[rows, cols] = dot(0, rows, cols) + dot(1, rows, cols) + dot(2, rows, cols)

    def away(start, size):
        rows = pl.ds(start, size)

        @pl.loop(0, width // FAR_TILE_N)
        def _(tile):
            cols = pl.ds(pl.multiple_of(tile * FAR_TILE_N, FAR_TILE_N), FAR_TILE_N)
            c_ref[rows, cols] = (acc[rows, cols] + dot(3, rows, cols)).astype(c_ref.dtype)

    quarter = rows_a // (4 * BLOCK)
    for first, second in ((1, 2), (0, 3)):
        if first == 0:
            for way in range(2):
                a_own(way, 3).wait_recv()

        @pl.loop(0, 2 * quarter)
        def _(turn):
            near(first * quarter + turn % quarter + (turn // quarter) * (second - first) * quarter)

    for way in range(2):
        for k in range(4):
            a_own(way, k).wait_send()
        for part in range(2):
            b_own(way, part).wait_send()
        b_far(way).wait_send()
    for slot in range(4):
        for part in range(2):
            b_share(slot, part).wait_send()

    for k in range(pieces):
        for way in range(2):
            a_far(way, k).wait_recv()
            if k < pieces - 2:
                away(*far[way][k])
    for k in range(pieces - 1):
        for way in range(2):
            a_far(way, k).wait_send()
    spared(lambda copy: copy.wait_send())


def finish(num_cols, c_done, a_all, b_all, acc, c_hbm, c_last, sems):
    rows_c = c_hbm.shape[0]
    mid = rows_c // 2
    tail = pl.ds(mid - LAST, 2 * LAST)
    copies = []
    for k, rows in enumerate((pl.ds(0, mid - LAST), pl.ds(mid + LAST, mid - LAST))):
        copies.append(pltpu.make_async_copy(c_done.at[rows], c_hbm.at[rows], sems.at[k]))
        copies[-1].start(priority=k)
    block = (lax.axis_index("col") + 2) % num_cols
    c_last[...] = (acc[tail] + jnp.dot(a_all[3, tail, :], b_all[block], preferred_element_type=jnp.float32)).astype(c_last.dtype)
    copies.append(pltpu.make_async_copy(c_last, c_hbm.at[tail], sems.at[2]))
    copies[-1].start()
    for copy in copies:
        copy.wait()


def solution(mesh):
    num_rows, num_cols = mesh.shape["row"], mesh.shape["col"]

    def local_product(a_blk, b_blk):
        rows, depth = a_blk.shape
        depth_b, width = b_blk.shape
        dma = pltpu.SemaphoreType.DMA
        vmem = pl.BlockSpec(memory_space=pltpu.VMEM)
        hbm = pl.BlockSpec(memory_space=pltpu.HBM)
        far_flops = 4 * LAST * width * depth
        pieces = len(far_plan(rows)[0])
        gathered = pl.pallas_call(
            functools.partial(gather_multiply, num_rows, num_cols),
            out_shape=(
                pltpu.VMEM((rows, width), jnp.bfloat16),
                pltpu.VMEM((4, rows, depth), jnp.bfloat16),
                pltpu.VMEM((num_rows // 2, 2 * depth_b, width), jnp.bfloat16),
                pltpu.VMEM((rows, width), jnp.float32),
            ),
            in_specs=[hbm] * 2,
            out_specs=(vmem,) * 4,
            scratch_shapes=[
                dma((2, 2)),
                dma((2,)),
                dma((2, 4)),
                dma((2, 4)),
                dma((2, pieces)),
                dma((2, pieces)),
                dma((2,)),
                dma((2, 2)),
                dma((2, 2)),
                dma((2,)),
                dma((2,)),
                dma((4, 2)),
                dma((4, 2)),
                pltpu.SemaphoreType.REGULAR,
                pltpu.SemaphoreType.REGULAR,
                pltpu.SemaphoreType.REGULAR,
                pltpu.SemaphoreType.REGULAR,
            ],
            cost_estimate=pl.CostEstimate(flops=2 * rows * width * depth * num_cols - far_flops, bytes_accessed=2 * (rows * depth + depth_b * width), transcendentals=0),
            compiler_params=pltpu.CompilerParams(collective_id=0, has_side_effects=True, vmem_limit_bytes=8 * 1024 * 1024),
            name="gather_multiply",
        )(a_blk, b_blk)
        return pl.pallas_call(
            functools.partial(finish, num_cols),
            out_shape=jax.ShapeDtypeStruct((rows, width), jnp.bfloat16),
            in_specs=[vmem] * 4,
            out_specs=hbm,
            scratch_shapes=[pltpu.VMEM((2 * LAST, width), jnp.bfloat16), dma((3,))],
            cost_estimate=pl.CostEstimate(flops=far_flops, bytes_accessed=2 * rows * width, transcendentals=0),
            compiler_params=pltpu.CompilerParams(vmem_limit_bytes=8 * 1024 * 1024),
            name="finish",
        )(*(pltpu.with_memory_space_constraint(part, pltpu.VMEM) for part in gathered))

    return jax.shard_map(local_product, mesh=mesh, in_specs=(P(("dp", "row"), "col"), P("row", "col")), out_specs=P(("dp", "row"), "col"), check_vma=False)
```

```python
import functools

import jax
import jax.numpy as jnp
from jax import lax
from jax.experimental import pallas as pl
from jax.experimental.pallas import tpu as pltpu
from jax.sharding import PartitionSpec as P

MESH = pl.DeviceIdType.MESH
BLOCK = 512
PIECE = 256
LAST = 128
SPARED = (40, 32)
TILE_N = 512
FAR_TILE_N = 1024


def own_plan(rows):
    mid = rows // 2
    return (
        ((0, LAST), (LAST, mid - LAST), (mid, mid // 2), (mid + mid // 2, mid // 2)),
        ((rows - LAST, LAST), (mid, mid - LAST), (mid // 2, mid // 2), (0, mid // 2)),
    )


def far_plan(rows):
    mid = rows // 2
    plans = []
    for spared in SPARED:
        sizes = [PIECE] * (mid // PIECE - 1) + [LAST] * (PIECE // LAST - 1) + [LAST - spared, spared]
        plans.append([(sum(sizes[:k]), size) for k, size in enumerate(sizes)])
    return plans[0], [(rows - start - size, size) for start, size in plans[1]]


def gather_multiply(num_rows, num_cols, a_hbm, b_hbm, c_ref, a_all, b_all, acc, la, lb, asend, arecv, fsend, frecv, esend, bsend, brecv, gsend, grecv, psend, precv, peer, joined, ready, go):
    row, col = lax.axis_index("row"), lax.axis_index("col")
    chip, core = row // 2, row % 2
    num_chips = num_rows // 2
    rows_a = a_hbm.shape[0]
    depth_b, width = b_hbm.shape
    own, far = own_plan(rows_a), far_plan(rows_a)
    pieces = len(far[0])
    half = depth_b // 2

    up, down = {"col": (col + 1) % num_cols}, {"col": (col + num_cols - 1) % num_cols}
    east, west = {"row": (row + 2) % num_rows}, {"row": (row + num_rows - 2) % num_rows}
    partner = {"row": row + 1 - 2 * core}
    a_dirs, b_dirs = (up, down), (east, west)

    def remote(src, dst, send, recv, device):
        return pltpu.make_async_remote_copy(src_ref=src, dst_ref=dst, send_sem=send, recv_sem=recv, device_id=device, device_id_type=MESH)

    def a_at(slot, place):
        return a_all.at[slot, pl.ds(*place)]

    def a_own(way, k):
        source = a_hbm.at[pl.ds(*own[way][0])] if k == 0 else a_at(0, own[way][k])
        return remote(source, a_at(1 + way, own[way][k]), asend.at[way, k], arecv.at[way, k], a_dirs[way])

    def a_far(way, k):
        return remote(a_at(1 + way, far[way][k]), a_at(3, far[way][k]), fsend.at[way, k], frecv.at[way, k], a_dirs[way])

    def a_extra(way):
        place = far[1 - way][-1]
        return remote(a_at(1 + way, place), a_at(3, place), esend.at[way], frecv.at[1 - way, pieces - 1], a_dirs[way])

    chip_at = (chip, (chip + num_chips - 1) % num_chips, (chip + 1) % num_chips, (chip + 2) % num_chips)

    def b_at(slot, side, part):
        return b_all.at[chip_at[slot], pl.ds(pl.multiple_of(side * depth_b + part * half, half), half)]

    def b_own(way, part):
        piece = b_at(0, core, part)
        return remote(piece, piece, bsend.at[way, part], brecv.at[way, part], b_dirs[way])

    def b_far(way):
        piece = b_at(1 + way, core, way)
        return remote(piece, piece, gsend.at[way], grecv.at[way], b_dirs[way])

    def b_share(slot, part):
        piece = b_at(slot, core, part)
        return remote(piece, piece, psend.at[slot, part], precv.at[slot, part], partner)

    def a_load(way, k):
        return pltpu.make_async_copy(a_hbm.at[pl.ds(*own[way][k])], a_at(0, own[way][k]), la.at[way, k])

    def b_load(part):
        return pltpu.make_async_copy(b_hbm.at[pl.ds(part * half, half)], b_at(0, core, part), lb.at[part])

    barrier = pltpu.get_barrier_semaphore()
    hub, after, across, before = range(num_cols)

    def signal(sem, *devices):
        for device in devices:
            pl.semaphore_signal(sem, inc=1, device_id=device, device_id_type=MESH)

    def send_own(way, between=None):
        a_own(way, 0).start()
        if between is None:
            a_own(1 - way, 0).start()
        for k in range(2):
            a_load(way, k).wait()
        a_own(way, 1).start()
        for k in range(2):
            a_load(1 - way, k).wait()
        for k in range(2, 4):
            a_own(way, k).start()
        if between is not None:
            between()
            a_own(1 - way, 0).start()
        for k in range(1, 4):
            a_own(1 - way, k).start()

    signal(barrier, up)

    @pl.when(col == hub)
    def _():
        signal(barrier, down, east, west, partner)

    for k in range(2):
        for way in range(2):
            a_load(way, k).start()

    @pl.when(jnp.logical_or(col == after, col == across))
    def _():
        pl.semaphore_wait(barrier, 1)
        signal(peer, down)
        send_own(1, lambda: pl.semaphore_wait(peer, 1))

    @pl.when(col == before)
    def _():
        pl.semaphore_wait(barrier, 2)
        signal(peer, down)
        send_own(0)

    @pl.when(col == hub)
    def _():
        pl.semaphore_wait(peer, 1)
        send_own(0, lambda: pl.semaphore_wait(barrier, 4))

    b_load(0).start()
    b_load(1).start()

    @pl.when(col == hub)
    def _():
        pl.semaphore_wait(joined, 2)
        signal(ready, east, west, partner)
        pl.semaphore_wait(ready, 3)
        signal(go, up, down)

    @pl.when(col == before)
    def _():
        signal(joined, up)
        pl.semaphore_wait(go, 1)

    @pl.when(col == after)
    def _():
        signal(joined, down)
        pl.semaphore_wait(go, 1)
        signal(go, up)

    @pl.when(col == across)
    def _():
        pl.semaphore_wait(go, 1)

    b_load(0).wait()
    b_load(1).wait()
    for part in range(2):
        b_own(0, part).start()
        b_own(1, 1 - part).start()
    for part in range(2):
        b_share(0, part).start()

    for way in range(2):
        b_own(way, way).wait_recv()
        b_far(way).start()
        b_share(1 + way, way).start()

    for way in range(2):
        for k in range(2):
            a_own(way, k).wait_recv()
        for k in range(pieces - 1):
            a_far(way, k).start()

    for way in range(2):
        b_own(way, 1 - way).wait_recv()
        b_share(1 + way, 1 - way).start()
    for way in range(2):
        b_far(way).wait_recv()
        b_share(3, way).start()
    for slot in range(4):
        for part in range(2):
            b_share(slot, part).wait_recv()

    for way in range(2):
        a_own(way, 2).wait_recv()

    def spared(act):
        @pl.when(col != before)
        def _():
            act(a_far(0, pieces - 1))

        @pl.when(col != hub)
        def _():
            act(a_far(1, pieces - 1))

        @pl.when(col == after)
        def _():
            act(a_extra(1))

        @pl.when(col == across)
        def _():
            act(a_extra(0))

    spared(lambda copy: copy.start())

    block_at = (col, (col + num_cols - 1) % num_cols, (col + 1) % num_cols, (col + 2) % num_cols)

    def dot(slot, rows, cols):
        return jnp.dot(a_all[slot, rows, :], b_all[block_at[slot], :, cols], preferred_element_type=jnp.float32)

    def near(block):
        rows = pl.ds(pl.multiple_of(block * BLOCK, BLOCK), BLOCK)

        @pl.loop(0, width // TILE_N)
        def _(tile):
            cols = pl.ds(pl.multiple_of(tile * TILE_N, TILE_N), TILE_N)
            acc[rows, cols] = dot(0, rows, cols) + dot(1, rows, cols) + dot(2, rows, cols)

    def away(start, size):
        rows = pl.ds(start, size)

        @pl.loop(0, width // FAR_TILE_N)
        def _(tile):
            cols = pl.ds(pl.multiple_of(tile * FAR_TILE_N, FAR_TILE_N), FAR_TILE_N)
            c_ref[rows, cols] = (acc[rows, cols] + dot(3, rows, cols)).astype(c_ref.dtype)

    quarter = rows_a // (4 * BLOCK)
    for first, second in ((1, 2), (0, 3)):
        if first == 0:
            for way in range(2):
                a_own(way, 3).wait_recv()

        @pl.loop(0, 2 * quarter)
        def _(turn):
            near(first * quarter + turn % quarter + (turn // quarter) * (second - first) * quarter)

    for way in range(2):
        for k in range(4):
            a_own(way, k).wait_send()
        for part in range(2):
            b_own(way, part).wait_send()
        b_far(way).wait_send()
    for slot in range(4):
        for part in range(2):
            b_share(slot, part).wait_send()

    for k in range(pieces):
        for way in range(2):
            a_far(way, k).wait_recv()
            if k < pieces - 2:
                away(*far[way][k])
    for k in range(pieces - 1):
        for way in range(2):
            a_far(way, k).wait_send()
    spared(lambda copy: copy.wait_send())


def finish(num_cols, c_done, a_all, b_all, acc, c_hbm, c_last, sems):
    rows_c = c_hbm.shape[0]
    mid = rows_c // 2
    tail = pl.ds(mid - LAST, 2 * LAST)
    copies = []
    for k, rows in enumerate((pl.ds(0, mid - LAST), pl.ds(mid + LAST, mid - LAST))):
        copies.append(pltpu.make_async_copy(c_done.at[rows], c_hbm.at[rows], sems.at[k]))
        copies[-1].start(priority=k)
    block = (lax.axis_index("col") + 2) % num_cols
    c_last[...] = (acc[tail] + jnp.dot(a_all[3, tail, :], b_all[block], preferred_element_type=jnp.float32)).astype(c_last.dtype)
    copies.append(pltpu.make_async_copy(c_last, c_hbm.at[tail], sems.at[2]))
    copies[-1].start()
    for copy in copies:
        copy.wait()


def solution(mesh):
    num_rows, num_cols = mesh.shape["row"], mesh.shape["col"]

    def local_product(a_blk, b_blk):
        rows, depth = a_blk.shape
        depth_b, width = b_blk.shape
        dma = pltpu.SemaphoreType.DMA
        vmem = pl.BlockSpec(memory_space=pltpu.VMEM)
        hbm = pl.BlockSpec(memory_space=pltpu.HBM)
        far_flops = 4 * LAST * width * depth
        pieces = len(far_plan(rows)[0])
        gathered = pl.pallas_call(
            functools.partial(gather_multiply, num_rows, num_cols),
            out_shape=(
                pltpu.VMEM((rows, width), jnp.bfloat16),
                pltpu.VMEM((4, rows, depth), jnp.bfloat16),
                pltpu.VMEM((num_rows // 2, 2 * depth_b, width), jnp.bfloat16),
                pltpu.VMEM((rows, width), jnp.float32),
            ),
            in_specs=[hbm] * 2,
            out_specs=(vmem,) * 4,
            scratch_shapes=[
                dma((2, 2)),
                dma((2,)),
                dma((2, 4)),
                dma((2, 4)),
                dma((2, pieces)),
                dma((2, pieces)),
                dma((2,)),
                dma((2, 2)),
                dma((2, 2)),
                dma((2,)),
                dma((2,)),
                dma((4, 2)),
                dma((4, 2)),
                pltpu.SemaphoreType.REGULAR,
                pltpu.SemaphoreType.REGULAR,
                pltpu.SemaphoreType.REGULAR,
                pltpu.SemaphoreType.REGULAR,
            ],
            cost_estimate=pl.CostEstimate(flops=2 * rows * width * depth * num_cols - far_flops, bytes_accessed=2 * (rows * depth + depth_b * width), transcendentals=0),
            compiler_params=pltpu.CompilerParams(collective_id=0, has_side_effects=True, vmem_limit_bytes=8 * 1024 * 1024),
            name="gather_multiply",
        )(a_blk, b_blk)
        return pl.pallas_call(
            functools.partial(finish, num_cols),
            out_shape=jax.ShapeDtypeStruct((rows, width), jnp.bfloat16),
            in_specs=[vmem] * 4,
            out_specs=hbm,
            scratch_shapes=[pltpu.VMEM((2 * LAST, width), jnp.bfloat16), dma((3,))],
            cost_estimate=pl.CostEstimate(flops=far_flops, bytes_accessed=2 * rows * width, transcendentals=0),
            compiler_params=pltpu.CompilerParams(vmem_limit_bytes=8 * 1024 * 1024),
            name="finish",
        )(*(pltpu.with_memory_space_constraint(part, pltpu.VMEM) for part in gathered))

    return jax.shard_map(local_product, mesh=mesh, in_specs=(P(("dp", "row"), "col"), P("row", "col")), out_specs=P(("dp", "row"), "col"), check_vma=False)
```
